32 devices in a mesh: ea: 8 (over z, x), sa: 4 (over y, core).
Axes of the slice: x: 2, y: 2, z: 4, core: 2. Of those that a mesh axis runs over, the one named last changes fastest.
Arguments:
- expert_hidden: bfloat16 [32, 1792, 512], P('ea', 'sa'), may hold values from -6 to 6
- down_weight: bfloat16 [32, 512, 2048], P('ea'), may hold values from -0.25 to 0.25
- residual: bfloat16 [8, 512, 2048], P('ea', 'sa'), may hold values from -6 to 6
- expert_ids: int32 [8, 512, 10], P('ea', 'sa'), may hold values from 0 to 31, all different within a row; in each aligned block of 128 rows (0 to 127, 128 to 255, ..., all dimensions but the last counted through in order) at most 56 rows name the same one
- combine_weight: float32 [8, 512, 10], P('ea', 'sa'), may hold values from 0.05 to 0.3
- norm_gain: bfloat16 [2048], replicated, may hold values from 0.25 to 1.75
- value_weight: bfloat16 [2048, 2048], P('ea'), may hold values from -0.125 to 0.125
- queries: bfloat16 [8, 512, 1024], P('ea', 'sa'), may hold values from -6 to 6
- keys: bfloat16 [8, 512, 1024], P('ea', 'sa'), may hold values from -6 to 6
- log_decay: float32 [8, 512, 16], P('ea', 'sa'), may hold values from -1 to 0, as said below
- write_rate: float32 [8, 512, 16], P('ea', 'sa'), may hold values from 0.1 to 0.9
Outputs:
- head_out: bfloat16 [8, 512, 2048], P('ea', 'sa')
The draws below stay inside these ranges and needn't reach their ends.
Inputs may be any that keep to these rules, and one draw needn't show every extreme that they name: `expert_ids`: each row names 10 different experts; among the rows of one device (aligned blocks of 128 rows) no expert is named more than 56 times, a bound that some block reaches. `log_decay`: below zero.
All inputs are finite; a program needn't handle non-finite values.
Results may differ from the reference program's by a relative error of at most 0.0066.
Values may be sent and summed in bfloat16 or wider, within the bound.
A program may use at most 128 MiB of HBM per device.

```python
import math
import jax
import jax.numpy as jnp
import numpy as np
from jax import lax

D = 2048
FF = 512
TOP = 10
HV = 16
HK = 8
DK = 128
DV = 128
TOK_DEV = 128
EXPERTS = 32
SEQS = 8
LEN = 512
CAP = 56
N_EA = 8
N_SA = 4


def draw_log_decay(key, part):
    k_fast, k_jitter, k_spots, k_drop = jax.random.split(key, 4)
    share = 0.5
    fast = jax.random.uniform(k_fast, (HV,)) < share
    slow_rate = 0.25 * math.log(10.0) / LEN
    base = jnp.where(fast, 1.0 / 40.0, slow_rate)
    jitter = jnp.exp(jax.random.uniform(k_jitter, (SEQS, LEN, HV), minval=-0.7, maxval=0.7))
    spots = jax.random.randint(k_spots, (SEQS, 2), 0, LEN)
    marked = jnp.any(jnp.arange(LEN)[None, :, None] == spots[:, None, :], axis=-1)
    drop = jnp.log(jax.random.uniform(k_drop, (SEQS, LEN), minval=0.5, maxval=0.8))
    final_result = -base[None, None, :] * jitter + jnp.where(marked, drop, 0.0)[:, :, None]
    return final_result.astype(jnp.float32)


def shard_levels(key, extent, pieces, smallest, top_value):
    level = 1.0
    for axis_at, parts in pieces:
        heights = jax.random.uniform(jax.random.fold_in(jax.random.fold_in(key, 6), axis_at), (parts,), jnp.float32, smallest / len(pieces), top_value / len(pieces))
        level = level * jnp.repeat(jnp.exp(heights), extent[axis_at] // parts).reshape((-1,) + (1,) * (len(extent) - 1 - axis_at))
    return level


def assign_block(own_key, own, number, rows, count, top, bound, lean):
    ranking = jax.random.permutation(own_key, count)
    crowded, ordinary = load_shares(count, rows * top, bound, lean, True), load_shares(count, rows * top, bound, lean, False)
    places = jnp.arange(count)

    def named(lengths, turn):
        used = int((lengths > 0).sum())
        fixed = max(1, used // 4)
        moved = fixed + (places - fixed + turn * (used - fixed)) % max(1, count - fixed)
        return jnp.zeros((count,), jnp.int32).at[ranking[jnp.where(places < fixed, places, moved)]].set(jnp.asarray(lengths, jnp.int32))

    lengths = jnp.where(number % 4 == 0, named(crowded, number // 4), named(ordinary, number - number // 4 - 1))
    mixed = jax.random.permutation(jax.random.fold_in(own, 3), count)
    source_of, receiver = mixed[0:count // 2 * 2:2], mixed[1:count // 2 * 2:2]
    room = jnp.minimum(lengths[source_of] - 1, bound - lengths[receiver]) // 2
    room = jnp.where((source_of == ranking[0]) | (receiver == ranking[0]) | (lengths[receiver] == 0), 0, jnp.maximum(room, 0))
    moved = jax.random.randint(jax.random.fold_in(own, 4), (count // 2,), 0, 1 << 20) % (room + 1)
    lengths = lengths.at[source_of].add(-moved).at[receiver].add(moved)
    members = jnp.searchsorted(jnp.cumsum(lengths), jnp.arange(rows * top), side="right").astype(jnp.int32)
    table = members.reshape(top, rows).T
    table = table[jax.random.permutation(jax.random.fold_in(own, 1), rows)]
    turn = jax.random.randint(jax.random.fold_in(own, 2), (rows, 1), 0, top)
    return jnp.take_along_axis(table, (jnp.arange(top)[None, :] + turn) % top, axis=1)


def load_shares(amount, total, limit, skew, full):
    portions = [(1 << 20) // math.isqrt(standing ** skew) + 1 for standing in range(1, amount + 1)]
    largest = limit if full else min(limit, max(-(-total // amount), total * portions[0] // sum(portions)))
    least = 1 if total - largest >= amount - 1 else 0
    given, spare = [largest] + [least] * (amount - 1), total - largest - least * (amount - 1)
    while spare > 0:
        movable = [i for i in range(1, amount) if given[i] < largest] or [i for i in range(1, amount) if given[i] < limit]
        pool, left = sum([portions[i] for i in movable]), spare
        for i in movable:
            extra = min(limit - given[i], max(1, left * portions[i] // pool), spare)
            given[i] = given[i] + extra
            spare = spare - extra
    return np.array(given)


def scatter_about(stream_key, extent, width, bound, cuts=(), kind=jnp.bfloat16):
    values = jax.random.normal(stream_key, extent, jnp.float32) * width
    if len(cuts) > 0:
        values = shard_levels(stream_key, extent, cuts, -0.22, 0.18) * values
    return jnp.clip(values, min=-bound, max=bound).astype(kind)


def setup_inputs(seed: int = 0) -> dict:
    key_of = jax.random.split(jax.random.key(seed), 12)
    expert_hidden = scatter_about(key_of[0], (EXPERTS, N_SA * N_EA * CAP, FF), 1.0, 6.0, ((0, 8), (1, 4)))
    down_weight = scatter_about(key_of[1], (EXPERTS, FF, D), FF ** -0.5, 0.25, ((0, 8),))
    residual = scatter_about(key_of[2], (SEQS, LEN, D), 1.0, 6.0, ((0, 8), (1, 4)))
    expert_ids_keys = jax.random.split(jax.random.fold_in(key_of[3], 1), SEQS * LEN // TOK_DEV)
    expert_ids_turns = jax.random.permutation(jax.random.fold_in(key_of[3], 3), SEQS * LEN // TOK_DEV)
    expert_ids = jax.vmap(lambda own, number: assign_block(jax.random.fold_in(key_of[3], 2), own, number, TOK_DEV, EXPERTS, TOP, CAP, 1))(expert_ids_keys, expert_ids_turns).reshape((SEQS, LEN, TOP))
    combine_weight = jnp.clip(0.05 + 0.25 * jax.random.uniform(key_of[4], (SEQS, LEN, TOP), jnp.float32) ** shard_levels(key_of[4], (SEQS, LEN, TOP), ((0, 8), (1, 4)), -0.2, 0.2), 0.05, 0.3)
    norm_gain = jnp.clip(1.0 + 0.15 * jax.random.normal(key_of[5], (D,), jnp.float32), 0.25, 1.75).astype(jnp.bfloat16)
    value_weight = scatter_about(key_of[6], (D, HV * DV), D ** -0.5, 0.125, ((0, 8),))
    queries = scatter_about(key_of[7], (SEQS, LEN, HK * DK), 1.0, 6.0, ((0, 8), (1, 4)))
    keys = scatter_about(key_of[8], (SEQS, LEN, HK * DK), 1.0, 6.0, ((0, 8), (1, 4)))
    log_decay = draw_log_decay(jax.random.fold_in(key_of[11], 71), 0)
    write_rate = jnp.clip(0.1 + 0.79999997 * jax.random.uniform(key_of[10], (SEQS, LEN, HV), jnp.float32) ** shard_levels(key_of[10], (SEQS, LEN, HV), ((0, 8), (1, 4)), -0.2, 0.2), 0.1, 0.9)
    return dict(expert_hidden=expert_hidden, down_weight=down_weight, residual=residual, expert_ids=expert_ids, combine_weight=combine_weight, norm_gain=norm_gain, value_weight=value_weight, queries=queries, keys=keys, log_decay=log_decay, write_rate=write_rate)


PRECISION_LEVEL = lax.Precision.HIGHEST

def block_slots(ids):
    onehot = (ids[:, :, None] == jnp.arange(EXPERTS, dtype=jnp.int32)[None, None, :]).astype(jnp.int32)
    counts = lax.optimization_barrier(jnp.sum(onehot, axis=1))
    prior = jnp.cumsum(counts, axis=0) - counts
    return lax.optimization_barrier(jnp.sum(onehot * prior[:, None, :], axis=-1)).astype(jnp.int32)

def unit_rows(field):
    return field * lax.rsqrt(lax.optimization_barrier(jnp.sum(field * field, axis=-1, keepdims=True)) + 1e-06)

def reference(expert_hidden, down_weight, residual, expert_ids, combine_weight, norm_gain, value_weight, queries, keys, log_decay, write_rate):
    down32 = down_weight.astype(jnp.float32)
    hidden5 = expert_hidden.reshape(EXPERTS, N_SA, N_EA, CAP, FF)
    per_seq = jnp.moveaxis(hidden5, 2, 0)

    def one_sequence(inputs):
        hid_seq, res_seq, ids_seq, weight_seq = inputs
        outs = jnp.einsum('ejcf,efd->ejcd', hid_seq.astype(jnp.float32), down32)
        flat = outs.reshape(EXPERTS * N_SA * CAP, D).astype(jnp.bfloat16)
        flat = lax.optimization_barrier(flat)
        ids_blocks = ids_seq.reshape(N_SA, TOK_DEV, TOP)
        slots = jax.vmap(block_slots)(ids_blocks)
        shard = jnp.arange(N_SA, dtype=jnp.int32)[:, None, None]
        rows = ((ids_blocks * N_SA + shard) * CAP + slots).reshape(LEN, TOP)
        picked = jnp.take(flat, rows, axis=0).astype(jnp.float32)
        moe = lax.optimization_barrier(jnp.sum(weight_seq[:, :, None] * picked, axis=1))
        return (res_seq.astype(jnp.float32) + moe).astype(jnp.bfloat16)
    stream = lax.map(one_sequence, (per_seq, residual, expert_ids, combine_weight))
    flow_float32 = lax.optimization_barrier(stream).astype(jnp.float32)
    normed = flow_float32 * lax.rsqrt(lax.optimization_barrier(jnp.mean(flow_float32 * flow_float32, axis=-1, keepdims=True)) + 1e-06) * norm_gain.astype(jnp.float32)
    normed = normed.astype(jnp.bfloat16)
    values = jnp.dot(normed.reshape(SEQS * LEN, D), value_weight, preferred_element_type=jnp.float32).astype(jnp.bfloat16)
    values = lax.optimization_barrier(values).astype(jnp.float32).reshape(SEQS, LEN, HV, DV)
    qn = unit_rows(queries.astype(jnp.float32).reshape(SEQS, LEN, HK, DK)) * DK ** (-0.5)
    kn = unit_rows(keys.astype(jnp.float32).reshape(SEQS, LEN, HK, DK))
    qn = jnp.repeat(qn, HV // HK, axis=2)
    kn = jnp.repeat(kn, HV // HK, axis=2)

    def advance(running_state, inputs):
        qt, kt, vt, at, bt = inputs
        alpha = jnp.exp(at)
        seen = jnp.einsum('shkv,shk->shv', running_state, kt, precision=PRECISION_LEVEL)
        delta = bt[..., None] * (vt - alpha[..., None] * seen)
        running_state = alpha[..., None, None] * running_state + kt[..., :, None] * delta[..., None, :]
        return (running_state, jnp.einsum('shkv,shk->shv', running_state, qt, precision=PRECISION_LEVEL))
    start = jnp.zeros((SEQS, HV, DK, DV), jnp.float32)
    inputs = (jnp.moveaxis(qn, 1, 0), jnp.moveaxis(kn, 1, 0), jnp.moveaxis(values, 1, 0), jnp.moveaxis(log_decay, 1, 0), jnp.moveaxis(write_rate, 1, 0))
    final, outs = lax.scan(advance, start, inputs)
    return jnp.moveaxis(outs, 0, 1).reshape(SEQS, LEN, HV * DV).astype(jnp.bfloat16)
```

```python
import functools

import jax
import jax.numpy as jnp
from jax import lax
from jax.experimental import pallas as pl
from jax.experimental.pallas import tpu as pltpu
from jax.sharding import PartitionSpec as P

HV = 16
HK = 8
DK = 128
DV = 128
F32 = jnp.float32
BF16 = jnp.bfloat16
VMEM_BYTES = 60 * 1024 * 1024


def dot1(a, b):
    return jnp.dot(a.astype(BF16), b.astype(BF16), preferred_element_type=F32)


def split(a):
    high = a.astype(BF16)
    return high, (a - high.astype(F32)).astype(BF16)


def dot3(a, b):
    ah, al = split(a)
    bh, bl = split(b)
    d = functools.partial(jnp.dot, preferred_element_type=F32)
    return d(ah, bh) + (d(ah, bl) + d(al, bh))


def iotas(rows, columns):
    return (
        lax.broadcasted_iota(jnp.int32, (rows, columns), 0),
        lax.broadcasted_iota(jnp.int32, (rows, columns), 1),
    )


def expert_kernel(exp_dev, n_seq, pad, hidden_ref, down_ref, named_ref, out_ref, mix_ref, made_ref):
    tokens, top = out_ref.shape[1], named_ref.shape[2] // 2
    width = out_ref.shape[2]

    @pl.when(pl.program_id(0) == 0)
    def _():
        first = lax.axis_index("ea") * exp_dev
        row, col = iotas(tokens, tokens)
        before = (row > col).astype(BF16)
        place = lax.broadcasted_iota(jnp.int32, (tokens, pad), 1).astype(F32)

        def mix(s, carry):
            named = named_ref[s]
            ids, weights = named[:, :top], named[:, top:]
            parts = []
            for e in range(exp_dev):
                hit = ids == (first + e).astype(F32)
                count = jnp.sum(hit.astype(F32), axis=1, keepdims=True)
                weight = jnp.sum(jnp.where(hit, weights, 0.0), axis=1, keepdims=True)
                slot = jnp.dot(
                    before,
                    jnp.broadcast_to(count, (tokens, pad)).astype(BF16),
                    preferred_element_type=F32,
                )
                parts.append(jnp.where((slot == place) & (count > 0.0), weight, 0.0))
            mix_ref[s] = jnp.concatenate(parts, axis=1).astype(BF16)
            return carry

        lax.fori_loop(0, n_seq, mix, 0)

    for e in range(exp_dev):
        made = jnp.dot(
            hidden_ref[e], down_ref[e], preferred_element_type=F32
        ).astype(BF16)
        made_ref[:, pl.ds(e * pad, pad), :] = made.reshape(n_seq, pad, width)

    def emit(s, carry):
        out_ref[s] = jnp.dot(mix_ref[s], made_ref[s], preferred_element_type=F32).astype(
            out_ref.dtype
        )
        return carry

    lax.fori_loop(0, n_seq, emit, 0)


def expert_partials(hidden, down, named, n_seq, tokens):
    exp_dev, rows, ff_units = hidden.shape
    width = down.shape[2]
    pad = rows // n_seq
    tile = min(width, 512)
    return pl.pallas_call(
        functools.partial(expert_kernel, exp_dev, n_seq, pad),
        grid=(width // tile,),
        out_shape=jax.ShapeDtypeStruct((n_seq, tokens, width), BF16),
        in_specs=[
            pl.BlockSpec((exp_dev, rows, ff_units), lambda n: (0, 0, 0)),
            pl.BlockSpec((exp_dev, ff_units, tile), lambda n: (0, 0, n)),
            pl.BlockSpec(named.shape, lambda n: (0, 0, 0)),
        ],
        out_specs=pl.BlockSpec((n_seq, tokens, tile), lambda n: (0, 0, n)),
        scratch_shapes=[
            pltpu.VMEM((n_seq, tokens, exp_dev * pad), BF16),
            pltpu.VMEM((n_seq, exp_dev * pad, tile), BF16),
        ],
        compiler_params=pltpu.CompilerParams(vmem_limit_bytes=VMEM_BYTES),
        cost_estimate=pl.CostEstimate(
            flops=2 * exp_dev * rows * width * (ff_units + tokens),
            bytes_accessed=2 * (hidden.size + down.size + n_seq * tokens * width),
            transcendentals=0,
        ),
        name="experts",
    )(hidden, down, named)


def maps_kernel(q_ref, k_ref, decay_ref, decay_t_ref, rate_ref, rate_t_ref, mn_ref, ga_ref, sum_ref, sum_t_ref):
    kh = pl.program_id(0)
    tokens = q_ref.shape[0]
    row, col = iotas(tokens, tokens)
    inclusive, strict = row >= col, row > col

    @pl.when(kh == 0)
    def _():
        exact = functools.partial(
            jnp.dot, precision=lax.Precision.HIGHEST, preferred_element_type=F32
        )
        sum_ref[...] = exact(inclusive.astype(F32), decay_ref[...])
        sum_t_ref[...] = exact(decay_t_ref[...], (row <= col).astype(F32))

    def unit(x):
        x = x.astype(F32)
        return x * lax.rsqrt(jnp.sum(x * x, axis=-1, keepdims=True) + 1e-06)

    kn = unit(k_ref[...])
    qn = unit(q_ref[...]) * DK ** (-0.5)
    kn_t = kn.T
    pairs = dot3(jnp.concatenate([kn, qn], axis=0), kn_t)
    kk, qk = pairs[:tokens], pairs[tokens:]
    per = HV // HK
    sums, rates = sum_ref[...], rate_ref[...]
    lane = lax.broadcasted_iota(jnp.int32, sums.shape, 1)
    levels = []
    size = 1
    while size < tokens:
        levels.append(size)
        size *= 2
    state = []
    for u in range(per):
        h = kh * per + u
        s_col = jnp.sum(jnp.where(lane == h, sums, 0.0), axis=1, keepdims=True)
        b_col = jnp.sum(jnp.where(lane == h, rates, 0.0), axis=1, keepdims=True)
        s_row, b_row = sum_t_ref[pl.ds(h, 1), :], rate_t_ref[pl.ds(h, 1), :]
        ratio = jnp.where(inclusive, jnp.exp(jnp.where(inclusive, s_col - s_row, 0.0)), 0.0)
        lower = jnp.where(strict, b_col * ratio * kk, 0.0)
        state.append([s_col, s_row, b_row, ratio, lower, (row == col).astype(F32)])
    for size in levels:
        joins = (row // (2 * size) == col // (2 * size)) & (row // size != col // size)
        for st in state:
            link = jnp.where(joins, st[4], 0.0)
            if size == 1:
                st[5] = st[5] - link
            else:
                st[5] = st[5] - dot3(st[5], dot3(link, st[5]))
    for u, (s_col, s_row, b_row, ratio, lower, inverse) in enumerate(state):
        last = s_row[:, tokens - 1 :]
        growth = jnp.exp(s_col)
        both = jnp.concatenate([qk * ratio, kn_t * jnp.exp(last - s_row)], axis=0)
        mn = dot3(both, inverse) * b_row
        base = jnp.concatenate(
            [growth * qn, jnp.where(row == col, jnp.exp(last), 0.0)], axis=0
        )
        ga = base - dot3(mn, growth * kn)
        mn_ref[u] = mn.astype(BF16)
        ga_ref[u] = ga.astype(BF16)


def head_maps(queries, keys, decay, rate):
    tokens = queries.shape[0]
    per = HV // HK
    whole = lambda shape: pl.BlockSpec(shape, lambda h: (0, 0))
    out = jax.ShapeDtypeStruct((HV, tokens + DK, DK), BF16)
    return pl.pallas_call(
        maps_kernel,
        grid=(HK,),
        out_shape=(out, out),
        in_specs=[
            pl.BlockSpec((tokens, DK), lambda h: (0, h)),
            pl.BlockSpec((tokens, DK), lambda h: (0, h)),
            whole((tokens, HV)),
            whole((HV, tokens)),
            whole((tokens, HV)),
            whole((HV, tokens)),
        ],
        out_specs=[pl.BlockSpec((per, tokens + DK, DK), lambda h: (h, 0, 0))] * 2,
        scratch_shapes=[pltpu.VMEM((tokens, HV), F32), pltpu.VMEM((HV, tokens), F32)],
        compiler_params=pltpu.CompilerParams(vmem_limit_bytes=VMEM_BYTES),
        cost_estimate=pl.CostEstimate(
            flops=HV * 64 * 2 * tokens * tokens * DK,
            bytes_accessed=6 * tokens * HV * DK * 2,
            transcendentals=HV * tokens * tokens,
        ),
        name="maps",
    )(queries, keys, decay, decay.T, rate, rate.T)


def value_kernel(res_ref, moe_ref, gain_ref, weight_ref, mn_ref, out_ref, state_ref, normed_ref):
    tokens = res_ref.shape[0]

    @pl.when(pl.program_id(0) == 0)
    def _():
        stream = (res_ref[...].astype(F32) + moe_ref[...].astype(F32)).astype(BF16).astype(F32)
        scale = lax.rsqrt(jnp.mean(stream * stream, axis=-1, keepdims=True) + 1e-06)
        normed_ref[...] = (stream * scale * gain_ref[...].astype(F32)).astype(BF16)

    values = jnp.dot(normed_ref[...], weight_ref[...], preferred_element_type=F32).astype(BF16)
    for u in range(mn_ref.shape[0]):
        both = jnp.dot(
            mn_ref[u], values[:, u * DV : (u + 1) * DV], preferred_element_type=F32
        )
        out_ref[:, u * DV : (u + 1) * DV] = both[:tokens]
        state_ref[u] = both[tokens:].astype(BF16)


def value_heads(residual, moe, gain, weight, mn):
    tokens, width = residual.shape
    per = 4
    tile = per * DV
    whole = lambda shape: pl.BlockSpec(shape, lambda n: (0, 0))
    return pl.pallas_call(
        value_kernel,
        grid=(HV // per,),
        out_shape=(
            jax.ShapeDtypeStruct((tokens, HV * DV), F32),
            jax.ShapeDtypeStruct((HV, DK, DV), BF16),
        ),
        in_specs=[
            whole((tokens, width)),
            whole((tokens, width)),
            whole((1, width)),
            pl.BlockSpec((width, tile), lambda n: (0, n)),
            pl.BlockSpec((per, tokens + DK, DK), lambda n: (n, 0, 0)),
        ],
        out_specs=[
            pl.BlockSpec((tokens, tile), lambda n: (0, n)),
            pl.BlockSpec((per, DK, DV), lambda n: (n, 0, 0)),
        ],
        scratch_shapes=[pltpu.VMEM((tokens, width), BF16)],
        compiler_params=pltpu.CompilerParams(vmem_limit_bytes=VMEM_BYTES),
        cost_estimate=pl.CostEstimate(
            flops=2 * tokens * width * HV * DV,
            bytes_accessed=2 * (weight.size + 6 * tokens * width),
            transcendentals=0,
        ),
        name="values",
    )(residual, moe, gain.reshape(1, width), weight, mn)


def close_kernel(maps_ref, states_ref, ga_ref, zero_ref, out_ref):
    n_sa, per = maps_ref.shape[:2]
    tokens = zero_ref.shape[0]
    here = lax.axis_index("sa")
    for u in range(per):
        state = jnp.zeros((DK, DV), F32)
        for i in range(n_sa - 1):
            new = states_ref[i, u].astype(F32)
            if i > 0:
                new = new + dot1(maps_ref[i, u], state)
            state = jnp.where(i < here, new, state)
        cols = slice(u * DV, (u + 1) * DV)
        out_ref[:, cols] = (zero_ref[:, cols] + dot1(ga_ref[u, :tokens], state)).astype(BF16)


def close_heads(maps, states, ga, zero):
    n_sa = maps.shape[0]
    tokens = zero.shape[0]
    per = 4
    gathered = pl.BlockSpec((n_sa, per, DK, DK), lambda n: (0, n, 0, 0))
    return pl.pallas_call(
        close_kernel,
        grid=(HV // per,),
        out_shape=jax.ShapeDtypeStruct((tokens, HV * DV), BF16),
        in_specs=[
            gathered,
            gathered,
            pl.BlockSpec((per, tokens + DK, DK), lambda n: (n, 0, 0)),
            pl.BlockSpec((tokens, per * DV), lambda n: (0, n)),
        ],
        out_specs=pl.BlockSpec((tokens, per * DV), lambda n: (0, n)),
        compiler_params=pltpu.CompilerParams(vmem_limit_bytes=VMEM_BYTES),
        cost_estimate=pl.CostEstimate(
            flops=HV * n_sa * 2 * DK * DK * DV,
            bytes_accessed=2 * (2 * maps.size + ga.size + 3 * zero.size),
            transcendentals=0,
        ),
        name="close",
    )(maps, states, ga, zero)


def on_device(
    expert_hidden,
    down_weight,
    residual,
    expert_ids,
    combine_weight,
    norm_gain,
    value_weight,
    queries,
    keys,
    log_decay,
    write_rate,
):
    n_ea = lax.axis_size("ea")
    exp_dev, rows, ff_units = expert_hidden.shape
    cap = rows // n_ea
    tokens = residual.shape[1]
    pad = -(-cap // 16) * 16
    hidden = jnp.pad(
        expert_hidden.reshape(exp_dev, n_ea, cap, ff_units), ((0, 0), (0, 0), (0, pad - cap), (0, 0))
    ).reshape(exp_dev, n_ea * pad, ff_units)
    named = jnp.concatenate([expert_ids[0].astype(F32), combine_weight[0]], axis=-1)
    named = lax.all_gather(named, "ea")
    weight = lax.all_gather(value_weight, "ea", axis=0, tiled=True)
    partial = expert_partials(hidden, down_weight, named, n_ea, tokens)
    moe = lax.psum_scatter(partial, "ea", scatter_dimension=0, tiled=True)[0]
    mn, ga = head_maps(queries[0], keys[0], log_decay[0], write_rate[0])
    maps = lax.all_gather(ga[:, tokens:], "sa")
    zero, state = value_heads(residual[0], moe, norm_gain, weight, mn)
    states = lax.all_gather(state, "sa")
    return close_heads(maps, states, ga, zero)[None]


def solution(mesh):
    return jax.shard_map(
        on_device,
        mesh=mesh,
        in_specs=(
            P("ea", "sa", None),
            P("ea", None, None),
            P("ea", "sa", None),
            P("ea", "sa", None),
            P("ea", "sa", None),
            P(),
            P("ea", None),
            P("ea", "sa", None),
            P("ea", "sa", None),
            P("ea", "sa", None),
            P("ea", "sa", None),
        ),
        out_specs=P("ea", "sa", None),
        check_vma=False,
    )
```

```python
import functools

import jax
import jax.numpy as jnp
from jax import lax
from jax.experimental import pallas as pl
from jax.experimental.pallas import tpu as pltpu
from jax.sharding import PartitionSpec as P

HV = 16
HK = 8
DK = 128
DV = 128
F32 = jnp.float32
BF16 = jnp.bfloat16
VMEM_BYTES = 60 * 1024 * 1024
MESH = pl.DeviceIdType.MESH


def dot1(a, b):
    return jnp.dot(a.astype(BF16), b.astype(BF16), preferred_element_type=F32)


def split(a):
    high = a.astype(BF16)
    return high, (a - high.astype(F32)).astype(BF16)


def dot3(a, b):
    ah, al = split(a)
    bh, bl = split(b)
    d = functools.partial(jnp.dot, preferred_element_type=F32)
    return d(ah, bh) + (d(ah, bl) + d(al, bh))


def iotas(rows, columns):
    return (
        lax.broadcasted_iota(jnp.int32, (rows, columns), 0),
        lax.broadcasted_iota(jnp.int32, (rows, columns), 1),
    )


def expert_kernel(exp_dev, n_seq, pad, hidden_ref, down_ref, named_ref, out_ref, mix_ref, made_ref):
    tokens, top = out_ref.shape[1], named_ref.shape[2] // 2
    width = out_ref.shape[2]

    @pl.when(pl.program_id(0) == 0)
    def _():
        first = lax.axis_index("ea") * exp_dev
        row, col = iotas(tokens, tokens)
        before = (row > col).astype(BF16)
        place = lax.broadcasted_iota(jnp.int32, (tokens, pad), 1).astype(F32)

        def mix(s, carry):
            named = named_ref[s]
            ids, weights = named[:, :top], named[:, top:]
            parts = []
            for e in range(exp_dev):
                hit = ids == (first + e).astype(F32)
                count = jnp.sum(hit.astype(F32), axis=1, keepdims=True)
                weight = jnp.sum(jnp.where(hit, weights, 0.0), axis=1, keepdims=True)
                slot = jnp.dot(
                    before,
                    jnp.broadcast_to(count, (tokens, pad)).astype(BF16),
                    preferred_element_type=F32,
                )
                parts.append(jnp.where((slot == place) & (count > 0.0), weight, 0.0))
            mix_ref[s] = jnp.concatenate(parts, axis=1).astype(BF16)
            return carry

        lax.fori_loop(0, n_seq, mix, 0)

    for e in range(exp_dev):
        made = jnp.dot(
            hidden_ref[e], down_ref[e], preferred_element_type=F32
        ).astype(BF16)
        made_ref[:, pl.ds(e * pad, pad), :] = made.reshape(n_seq, pad, width)

    def emit(s, carry):
        out_ref[s] = jnp.dot(mix_ref[s], made_ref[s], preferred_element_type=F32).astype(
            out_ref.dtype
        )
        return carry

    lax.fori_loop(0, n_seq, emit, 0)


def expert_partials(hidden, down, named, n_seq, tokens):
    exp_dev, rows, ff_units = hidden.shape
    width = down.shape[2]
    pad = rows // n_seq
    tile = min(width, 512)
    return pl.pallas_call(
        functools.partial(expert_kernel, exp_dev, n_seq, pad),
        grid=(width // tile,),
        out_shape=jax.ShapeDtypeStruct((n_seq, tokens, width), BF16),
        in_specs=[
            pl.BlockSpec((exp_dev, rows, ff_units), lambda n: (0, 0, 0)),
            pl.BlockSpec((exp_dev, ff_units, tile), lambda n: (0, 0, n)),
            pl.BlockSpec(named.shape, lambda n: (0, 0, 0)),
        ],
        out_specs=pl.BlockSpec((n_seq, tokens, tile), lambda n: (0, 0, n)),
        scratch_shapes=[
            pltpu.VMEM((n_seq, tokens, exp_dev * pad), BF16),
            pltpu.VMEM((n_seq, exp_dev * pad, tile), BF16),
        ],
        compiler_params=pltpu.CompilerParams(vmem_limit_bytes=VMEM_BYTES),
        cost_estimate=pl.CostEstimate(
            flops=2 * exp_dev * rows * width * (ff_units + tokens),
            bytes_accessed=2 * (hidden.size + down.size + n_seq * tokens * width),
            transcendentals=0,
        ),
        name="experts",
    )(hidden, down, named)


def sum_decays(decay_ref, decay_t_ref, sum_ref, sum_t_ref):
    tokens = decay_ref.shape[0]
    row, col = iotas(tokens, tokens)
    exact = functools.partial(
        jnp.dot, precision=lax.Precision.HIGHEST, preferred_element_type=F32
    )
    sum_ref[...] = exact((row >= col).astype(F32), decay_ref[...])
    sum_t_ref[...] = exact(decay_t_ref[...], (row <= col).astype(F32))


def unit(x):
    x = x.astype(F32)
    return x * lax.rsqrt(jnp.sum(x * x, axis=-1, keepdims=True) + 1e-06)


def key_head_maps(kh, q, k, rate_ref, rate_t_ref, sum_ref, sum_t_ref):
    tokens = q.shape[0]
    row, col = iotas(tokens, tokens)
    inclusive, strict = row >= col, row > col
    kn = unit(k)
    qn = unit(q) * DK ** (-0.5)
    kn_t = kn.T
    pairs = dot3(jnp.concatenate([kn, qn], axis=0), kn_t)
    kk, qk = pairs[:tokens], pairs[tokens:]
    per = HV // HK
    sums, rates = sum_ref[...], rate_ref[...]
    lane = lax.broadcasted_iota(jnp.int32, sums.shape, 1)
    levels = []
    size = 1
    while size < tokens:
        levels.append(size)
        size *= 2
    state = []
    for u in range(per):
        h = kh * per + u
        s_col = jnp.sum(jnp.where(lane == h, sums, 0.0), axis=1, keepdims=True)
        b_col = jnp.sum(jnp.where(lane == h, rates, 0.0), axis=1, keepdims=True)
        s_row, b_row = sum_t_ref[pl.ds(h, 1), :], rate_t_ref[pl.ds(h, 1), :]
        ratio = jnp.where(inclusive, jnp.exp(jnp.where(inclusive, s_col - s_row, 0.0)), 0.0)
        lower = jnp.where(strict, b_col * ratio * kk, 0.0)
        state.append([s_col, s_row, b_row, ratio, lower, (row == col).astype(F32)])
    for size in levels:
        joins = (row // (2 * size) == col // (2 * size)) & (row // size != col // size)
        for st in state:
            link = jnp.where(joins, st[4], 0.0)
            if size == 1:
                st[5] = st[5] - link
            else:
                st[5] = st[5] - dot3(st[5], dot3(link, st[5]))
    outs = []
    for u, (s_col, s_row, b_row, ratio, lower, inverse) in enumerate(state):
        last = s_row[:, tokens - 1 :]
        growth = jnp.exp(s_col)
        both = jnp.concatenate([qk * ratio, kn_t * jnp.exp(last - s_row)], axis=0)
        mn = dot3(both, inverse) * b_row
        base = jnp.concatenate(
            [growth * qn, jnp.where(row == col, jnp.exp(last), 0.0)], axis=0
        )
        ga = base - dot3(mn, growth * kn)
        outs.append((mn.astype(BF16), ga.astype(BF16)))
    return outs


def maps_kernel(q_ref, k_ref, decay_ref, decay_t_ref, rate_ref, rate_t_ref, mn_ref, ga_ref, sum_ref, sum_t_ref):
    kh = pl.program_id(0)

    @pl.when(kh == 0)
    def _():
        sum_decays(decay_ref, decay_t_ref, sum_ref, sum_t_ref)

    outs = key_head_maps(kh, q_ref[...], k_ref[...], rate_ref, rate_t_ref, sum_ref, sum_t_ref)
    for u, (mn, ga) in enumerate(outs):
        mn_ref[u] = mn
        ga_ref[u] = ga


def head_maps(queries, keys, decay, rate):
    tokens = queries.shape[0]
    per = HV // HK
    whole = lambda shape: pl.BlockSpec(shape, lambda h: (0, 0))
    out = jax.ShapeDtypeStruct((HV, tokens + DK, DK), BF16)
    return pl.pallas_call(
        maps_kernel,
        grid=(HK,),
        out_shape=(out, out),
        in_specs=[
            pl.BlockSpec((tokens, DK), lambda h: (0, h)),
            pl.BlockSpec((tokens, DK), lambda h: (0, h)),
            whole((tokens, HV)),
            whole((HV, tokens)),
            whole((tokens, HV)),
            whole((HV, tokens)),
        ],
        out_specs=[pl.BlockSpec((per, tokens + DK, DK), lambda h: (h, 0, 0))] * 2,
        scratch_shapes=[pltpu.VMEM((tokens, HV), F32), pltpu.VMEM((HV, tokens), F32)],
        compiler_params=pltpu.CompilerParams(vmem_limit_bytes=VMEM_BYTES),
        cost_estimate=pl.CostEstimate(
            flops=HV * 64 * 2 * tokens * tokens * DK,
            bytes_accessed=6 * tokens * HV * DK * 2,
            transcendentals=HV * tokens * tokens,
        ),
        name="maps",
    )(queries, keys, decay, decay.T, rate, rate.T)


def value_kernel(res_ref, moe_ref, gain_ref, weight_ref, mn_ref, out_ref, state_ref, normed_ref):
    tokens = res_ref.shape[0]

    @pl.when(pl.program_id(0) == 0)
    def _():
        stream = (res_ref[...].astype(F32) + moe_ref[...].astype(F32)).astype(BF16).astype(F32)
        scale = lax.rsqrt(jnp.mean(stream * stream, axis=-1, keepdims=True) + 1e-06)
        normed_ref[...] = (stream * scale * gain_ref[...].astype(F32)).astype(BF16)

    values = jnp.dot(normed_ref[...], weight_ref[...], preferred_element_type=F32).astype(BF16)
    for u in range(mn_ref.shape[0]):
        both = jnp.dot(
            mn_ref[u], values[:, u * DV : (u + 1) * DV], preferred_element_type=F32
        )
        out_ref[:, u * DV : (u + 1) * DV] = both[:tokens]
        state_ref[u] = both[tokens:].astype(BF16)


def value_heads(residual, moe, gain, weight, mn):
    tokens, width = residual.shape
    per = 4
    tile = per * DV
    whole = lambda shape: pl.BlockSpec(shape, lambda n: (0, 0))
    return pl.pallas_call(
        value_kernel,
        grid=(HV // per,),
        out_shape=(
            jax.ShapeDtypeStruct((tokens, HV * DV), F32),
            jax.ShapeDtypeStruct((HV, DK, DV), BF16),
        ),
        in_specs=[
            whole((tokens, width)),
            whole((tokens, width)),
            whole((1, width)),
            pl.BlockSpec((width, tile), lambda n: (0, n)),
            pl.BlockSpec((per, tokens + DK, DK), lambda n: (n, 0, 0)),
        ],
        out_specs=[
            pl.BlockSpec((tokens, tile), lambda n: (0, n)),
            pl.BlockSpec((per, DK, DV), lambda n: (n, 0, 0)),
        ],
        scratch_shapes=[pltpu.VMEM((tokens, width), BF16)],
        compiler_params=pltpu.CompilerParams(vmem_limit_bytes=VMEM_BYTES),
        cost_estimate=pl.CostEstimate(
            flops=2 * tokens * width * HV * DV,
            bytes_accessed=2 * (weight.size + 6 * tokens * width),
            transcendentals=0,
        ),
        name="values",
    )(residual, moe, gain.reshape(1, width), weight, mn)


def close_kernel(maps_ref, states_ref, ga_ref, zero_ref, out_ref):
    n_sa, per = maps_ref.shape[:2]
    tokens = zero_ref.shape[0]
    here = lax.axis_index("sa")
    for u in range(per):
        state = jnp.zeros((DK, DV), F32)
        for i in range(n_sa - 1):
            new = states_ref[i, u].astype(F32)
            if i > 0:
                new = new + dot1(maps_ref[i, u], state)
            state = jnp.where(i < here, new, state)
        cols = slice(u * DV, (u + 1) * DV)
        out_ref[:, cols] = (zero_ref[:, cols] + dot1(ga_ref[u, :tokens], state)).astype(BF16)


def close_heads(maps, states, ga, zero):
    n_sa = maps.shape[0]
    tokens = zero.shape[0]
    per = 4
    gathered = pl.BlockSpec((n_sa, per, DK, DK), lambda n: (0, n, 0, 0))
    return pl.pallas_call(
        close_kernel,
        grid=(HV // per,),
        out_shape=jax.ShapeDtypeStruct((tokens, HV * DV), BF16),
        in_specs=[
            gathered,
            gathered,
            pl.BlockSpec((per, tokens + DK, DK), lambda n: (n, 0, 0)),
            pl.BlockSpec((tokens, per * DV), lambda n: (0, n)),
        ],
        out_specs=pl.BlockSpec((tokens, per * DV), lambda n: (0, n)),
        compiler_params=pltpu.CompilerParams(vmem_limit_bytes=VMEM_BYTES),
        cost_estimate=pl.CostEstimate(
            flops=HV * n_sa * 2 * DK * DK * DV,
            bytes_accessed=2 * (2 * maps.size + ga.size + 3 * zero.size),
            transcendentals=0,
        ),
        name="close",
    )(maps, states, ga, zero)


def gather_kernel(
    cap, pad,
    named_ref, hidden_hbm, down_hbm, res_ref, gain_ref, weight_ref, q_ref, k_ref,
    decay_ref, decay_t_ref, rate_ref, rate_t_ref,
    normed_ref, full_ref, mn_ref, ga_ref,
    table_ref, hidden_ref, down_ref, made_ref, mix_ref, send_ref, got_ref, sum_ref, sum_t_ref,
    load_sem, own_sem, sem_t, sem_w, sem_f, sem_p,
):
    n = lax.axis_size("ea")
    me, here = lax.axis_index("ea"), lax.axis_index("sa")
    partner = here + 1 - 2 * lax.rem(here, 2)
    half = weight_ref.shape[0] // 2
    mine = pl.ds(pl.multiple_of(lax.rem(here, 2) * half, half), half)
    exp_dev, tokens, width = down_hbm.shape[0], res_ref.shape[0], res_ref.shape[1]
    top = named_ref.shape[0] // 2
    tile = 512
    tiles = width // tile

    def peer(d):
        return lax.rem(me + d, n)

    def origin(d):
        return lax.rem(me + n - d, n)

    def remote(src, dst, sems, d, where):
        return pltpu.make_async_remote_copy(
            src_ref=src, dst_ref=dst, send_sem=sems.at[0, d], recv_sem=sems.at[1, d],
            device_id=where, device_id_type=MESH,
        )

    def table_copy(d):
        return remote(named_ref, table_ref.at[me], sem_t, d, {"ea": peer(d)})

    def weight_copy(d):
        return remote(weight_ref.at[mine], full_ref.at[me, mine], sem_w, d, {"ea": peer(d)})

    def forward_copy(d):
        block = full_ref.at[origin(d), mine]
        return remote(block, block, sem_f, d, {"sa": partner})

    def partial_copy(d):
        return remote(send_ref.at[peer(d)], got_ref.at[d], sem_p, d, {"ea": peer(d)})

    def each(action):
        def turn(d, carry):
            action(d)
            return carry

        lax.fori_loop(1, n, turn, 0)

    loads = []
    for e in range(exp_dev):
        loads.append((
            pltpu.make_async_copy(hidden_hbm.at[e], hidden_ref.at[e], load_sem.at[0, e]),
            pltpu.make_async_copy(down_hbm.at[e], down_ref.at[e], load_sem.at[1, e]),
        ))
        for copy in loads[-1]:
            copy.start()
    own = pltpu.make_async_copy(weight_ref, full_ref.at[me], own_sem)
    own.start()

    barrier = pltpu.get_barrier_semaphore()
    each(lambda d: pl.semaphore_signal(barrier, inc=1, device_id={"ea": peer(d)}, device_id_type=MESH))
    pl.semaphore_signal(barrier, inc=1, device_id={"sa": partner}, device_id_type=MESH)
    pl.semaphore_wait(barrier, n)

    each(lambda d: table_copy(d).start())
    each(lambda d: weight_copy(d).start())

    for e in range(exp_dev):
        for copy in loads[e]:
            copy.wait()
        if pad > cap:
            made_ref[:, e * pad + cap : (e + 1) * pad, :] = jnp.zeros((n, pad - cap, width), BF16)

        def project(t, carry):
            cols = pl.ds(pl.multiple_of(t * tile, tile), tile)
            made = jnp.dot(hidden_ref[e], down_ref[e, :, cols], preferred_element_type=F32)
            for s in range(n):
                made_ref[s, e * pad : e * pad + cap, cols] = made[s * cap : (s + 1) * cap].astype(BF16)
            return carry

        lax.fori_loop(0, tiles, project, 0)

    table_ref[me] = named_ref[...]
    row, col = iotas(tokens, tokens)
    after = (row < col).astype(BF16)
    place = lax.broadcasted_iota(jnp.int32, (pad, tokens), 0).astype(F32)

    def partial(d, carry):
        s = peer(d)

        @pl.when(d < n)
        def _():
            table_copy(n - d).wait_recv()

        named = table_ref[s]
        ids, weights = named[:top], named[top:]
        parts = []
        for e in range(exp_dev):
            hit = ids == (me * exp_dev + e).astype(F32)
            count = jnp.sum(hit.astype(F32), axis=0, keepdims=True)
            weight = jnp.sum(jnp.where(hit, weights, 0.0), axis=0, keepdims=True)
            slot = jnp.dot(
                jnp.broadcast_to(count, (pad, tokens)).astype(BF16), after, preferred_element_type=F32
            )
            parts.append(jnp.where((slot == place) & (count > 0.0), weight, 0.0))
        mix_ref[...] = jnp.concatenate(parts, axis=0).T.astype(BF16)

        def block(t, inner):
            cols = pl.ds(pl.multiple_of(t * tile, tile), tile)
            send_ref[s, :, cols] = jnp.dot(
                mix_ref[...], made_ref[s, :, cols], preferred_element_type=F32
            ).astype(BF16)
            return inner

        lax.fori_loop(0, tiles, block, 0)

        @pl.when(d < n)
        def _():
            partial_copy(d).start()

        return carry

    lax.fori_loop(1, n + 1, partial, 0)

    sum_decays(decay_ref, decay_t_ref, sum_ref, sum_t_ref)

    def maps(kh, carry):
        cols = pl.ds(pl.multiple_of(kh * DK, DK), DK)
        outs = key_head_maps(kh, q_ref[:, cols], k_ref[:, cols], rate_ref, rate_t_ref, sum_ref, sum_t_ref)
        for u, (mn, ga) in enumerate(outs):
            mn_ref[kh * (HV // HK) + u] = mn
            ga_ref[kh * (HV // HK) + u] = ga
        return carry

    lax.fori_loop(0, HK, maps, 0)

    def pass_on(d):
        weight_copy(d).wait_recv()
        forward_copy(d).start()

    each(pass_on)
    each(lambda d: partial_copy(d).wait_recv())

    def close(r, carry):
        rows = pl.ds(pl.multiple_of(r * 16, 16), 16)
        moe = send_ref[me, rows, :].astype(F32)
        for d in range(1, n):
            moe = moe + got_ref[d, rows, :].astype(F32)
        stream = (res_ref[rows, :].astype(F32) + moe).astype(BF16).astype(F32)
        scale = lax.rsqrt(jnp.mean(stream * stream, axis=-1, keepdims=True) + 1e-06)
        normed_ref[rows, :] = (stream * scale * gain_ref[...].astype(F32)).astype(BF16)
        return carry

    lax.fori_loop(0, tokens // 16, close, 0)
    own.wait()

    def finish(d):
        forward_copy(d).wait()
        table_copy(d).wait_send()
        weight_copy(d).wait_send()
        partial_copy(d).wait_send()

    each(finish)


def gather_stage(n, named, hidden, down, residual, gain, weight, queries, keys, decay, rate):
    exp_dev, rows, ff_units = hidden.shape
    tokens, width = residual.shape
    cap = rows // n
    pad = -(-cap // 16) * 16
    vmem = pl.BlockSpec(memory_space=pltpu.VMEM)
    hbm = pl.BlockSpec(memory_space=pl.ANY)
    maps = jax.ShapeDtypeStruct((HV, tokens + DK, DK), BF16)
    dma = pltpu.SemaphoreType.DMA
    return pl.pallas_call(
        functools.partial(gather_kernel, cap, pad),
        out_shape=(
            jax.ShapeDtypeStruct((tokens, width), BF16),
            jax.ShapeDtypeStruct((n,) + weight.shape, BF16),
            maps,
            maps,
        ),
        in_specs=[vmem, hbm, hbm] + [vmem] * 9,
        out_specs=[vmem, hbm, vmem, vmem],
        scratch_shapes=[
            pltpu.VMEM((n,) + named.shape, F32),
            pltpu.VMEM(hidden.shape, BF16),
            pltpu.VMEM(down.shape, BF16),
            pltpu.VMEM((n, exp_dev * pad, width), BF16),
            pltpu.VMEM((tokens, exp_dev * pad), BF16),
            pltpu.VMEM((n, tokens, width), BF16),
            pltpu.VMEM((n, tokens, width), BF16),
            pltpu.VMEM((tokens, HV), F32),
            pltpu.VMEM((HV, tokens), F32),
            dma((2, exp_dev)),
            dma,
            dma((2, n)),
            dma((2, n)),
            dma((2, n)),
            dma((2, n)),
        ],
        compiler_params=pltpu.CompilerParams(
            vmem_limit_bytes=VMEM_BYTES, collective_id=0, has_side_effects=True
        ),
        name="gather",
    )(named, hidden, down, residual, gain.reshape(1, width), weight, queries, keys, decay, decay.T, rate, rate.T)


def chain_kernel(normed_ref, weight_ref, mn_ref, ga_ref, out_ref, send_ref, got_ref, sem):
    g, groups = pl.program_id(0), pl.num_programs(0)
    n, here = lax.axis_size("sa"), lax.axis_index("sa")
    tokens = normed_ref.shape[0]
    per = mn_ref.shape[0]
    following, previous = lax.rem(here + 1, n), lax.rem(here + n - 1, n)

    @pl.when(g == 0)
    def _():
        barrier = pltpu.get_barrier_semaphore()
        for where in (following, previous):
            pl.semaphore_signal(barrier, inc=1, device_id={"sa": where}, device_id_type=MESH)
        pl.semaphore_wait(barrier, 2)
        got_ref_first = jnp.zeros(got_ref.shape[1:], BF16)

        @pl.when(here == 0)
        def _():
            for i in range(got_ref.shape[0]):
                got_ref[i] = got_ref_first

    def copy(i):
        return pltpu.make_async_remote_copy(
            src_ref=send_ref.at[i], dst_ref=got_ref.at[i], send_sem=sem.at[0, i],
            recv_sem=sem.at[1, i], device_id={"sa": following}, device_id_type=MESH,
        )

    values = jnp.dot(normed_ref[...], weight_ref[...], preferred_element_type=F32).astype(BF16)
    both = [
        jnp.dot(mn_ref[u], values[:, u * DV : (u + 1) * DV], preferred_element_type=F32)
        for u in range(per)
    ]

    @pl.when(here > 0)
    def _():
        copy(g).wait_recv()

    after = [
        both[u] + jnp.dot(ga_ref[u], got_ref[g, u], preferred_element_type=F32) for u in range(per)
    ]
    for u in range(per):
        send_ref[g, u] = after[u][tokens:].astype(BF16)

    @pl.when(here < n - 1)
    def _():
        copy(g).start()

    for u in range(per):
        out_ref[:, u * DV : (u + 1) * DV] = after[u][:tokens].astype(BF16)

    @pl.when((g == groups - 1) & (here < n - 1))
    def _():
        for i in range(send_ref.shape[0]):
            copy(i).wait_send()


def chain_stage(normed, weight, mn, ga):
    tokens, width = normed.shape
    per = 4
    groups = HV // per
    tile = per * DV
    states = pltpu.VMEM((groups, per, DK, DV), BF16)
    maps = pl.BlockSpec((per, tokens + DK, DK), lambda g: (g, 0, 0))
    return pl.pallas_call(
        chain_kernel,
        grid=(groups,),
        out_shape=jax.ShapeDtypeStruct((tokens, HV * DV), BF16),
        in_specs=[
            pl.BlockSpec((tokens, width), lambda g: (0, 0)),
            pl.BlockSpec((width, tile), lambda g: (0, g)),
            maps,
            maps,
        ],
        out_specs=pl.BlockSpec((tokens, tile), lambda g: (0, g)),
        scratch_shapes=[states, states, pltpu.SemaphoreType.DMA((2, groups))],
        compiler_params=pltpu.CompilerParams(
            vmem_limit_bytes=VMEM_BYTES, collective_id=1, has_side_effects=True
        ),
        name="chain",
    )(normed, weight, mn, ga)


def on_device(
    expert_hidden,
    down_weight,
    residual,
    expert_ids,
    combine_weight,
    norm_gain,
    value_weight,
    queries,
    keys,
    log_decay,
    write_rate,
):
    n_ea = lax.axis_size("ea")
    exp_dev, rows, ff_units = expert_hidden.shape
    cap = rows // n_ea
    tokens = residual.shape[1]
    named = jnp.concatenate([expert_ids[0].astype(F32), combine_weight[0]], axis=-1)
    fits = n_ea * tokens * residual.shape[2] <= 4 * 1024 * 1024 and cap % 8 == 0
    if fits and lax.axis_size("sa") % 2 == 0:
        normed, weight, mn, ga = gather_stage(
            n_ea, named.T, expert_hidden, down_weight, residual[0], norm_gain, value_weight,
            queries[0], keys[0], log_decay[0], write_rate[0],
        )
        return chain_stage(normed, weight.reshape(-1, weight.shape[2]), mn, ga)[None]
    pad = -(-cap // 16) * 16
    hidden = jnp.pad(
        expert_hidden.reshape(exp_dev, n_ea, cap, ff_units), ((0, 0), (0, 0), (0, pad - cap), (0, 0))
    ).reshape(exp_dev, n_ea * pad, ff_units)
    named = lax.all_gather(named, "ea")
    weight = lax.all_gather(value_weight, "ea", axis=0, tiled=True)
    partial = expert_partials(hidden, down_weight, named, n_ea, tokens)
    moe = lax.psum_scatter(partial, "ea", scatter_dimension=0, tiled=True)[0]
    mn, ga = head_maps(queries[0], keys[0], log_decay[0], write_rate[0])
    maps = lax.all_gather(ga[:, tokens:], "sa")
    zero, state = value_heads(residual[0], moe, norm_gain, weight, mn)
    states = lax.all_gather(state, "sa")
    return close_heads(maps, states, ga, zero)[None]


def solution(mesh):
    return jax.shard_map(
        on_device,
        mesh=mesh,
        in_specs=(
            P("ea", "sa", None),
            P("ea", None, None),
            P("ea", "sa", None),
            P("ea", "sa", None),
            P("ea", "sa", None),
            P(),
            P("ea", None),
            P("ea", "sa", None),
            P("ea", "sa", None),
            P("ea", "sa", None),
            P("ea", "sa", None),
        ),
        out_specs=P("ea", "sa", None),
        check_vma=False,
    )
```

```python
import functools

import jax
import jax.numpy as jnp
from jax import lax
from jax.experimental import pallas as pl
from jax.experimental.pallas import tpu as pltpu
from jax.sharding import PartitionSpec as P

HV = 16
HK = 8
DK = 128
DV = 128
F32 = jnp.float32
BF16 = jnp.bfloat16
VMEM_BYTES = 60 * 1024 * 1024
MESH = pl.DeviceIdType.MESH


def dot1(a, b):
    return jnp.dot(a.astype(BF16), b.astype(BF16), preferred_element_type=F32)


def split(a):
    high = a.astype(BF16)
    return high, (a - high.astype(F32)).astype(BF16)


def dot3(a, b):
    ah, al = split(a)
    bh, bl = split(b)
    d = functools.partial(jnp.dot, preferred_element_type=F32)
    return d(ah, bh) + (d(ah, bl) + d(al, bh))


def iotas(rows, columns):
    return (
        lax.broadcasted_iota(jnp.int32, (rows, columns), 0),
        lax.broadcasted_iota(jnp.int32, (rows, columns), 1),
    )


def expert_kernel(exp_dev, n_seq, pad, hidden_ref, down_ref, named_ref, out_ref, mix_ref, made_ref):
    tokens, top = out_ref.shape[1], named_ref.shape[2] // 2
    width = out_ref.shape[2]

    @pl.when(pl.program_id(0) == 0)
    def _():
        first = lax.axis_index("ea") * exp_dev
        row, col = iotas(tokens, tokens)
        before = (row > col).astype(BF16)
        place = lax.broadcasted_iota(jnp.int32, (tokens, pad), 1).astype(F32)

        def mix(s, carry):
            named = named_ref[s]
            ids, weights = named[:, :top], named[:, top:]
            parts = []
            for e in range(exp_dev):
                hit = ids == (first + e).astype(F32)
                count = jnp.sum(hit.astype(F32), axis=1, keepdims=True)
                weight = jnp.sum(jnp.where(hit, weights, 0.0), axis=1, keepdims=True)
                slot = jnp.dot(
                    before,
                    jnp.broadcast_to(count, (tokens, pad)).astype(BF16),
                    preferred_element_type=F32,
                )
                parts.append(jnp.where((slot == place) & (count > 0.0), weight, 0.0))
            mix_ref[s] = jnp.concatenate(parts, axis=1).astype(BF16)
            return carry

        lax.fori_loop(0, n_seq, mix, 0)

    for e in range(exp_dev):
        made = jnp.dot(
            hidden_ref[e], down_ref[e], preferred_element_type=F32
        ).astype(BF16)
        made_ref[:, pl.ds(e * pad, pad), :] = made.reshape(n_seq, pad, width)

    def emit(s, carry):
        out_ref[s] = jnp.dot(mix_ref[s], made_ref[s], preferred_element_type=F32).astype(
            out_ref.dtype
        )
        return carry

    lax.fori_loop(0, n_seq, emit, 0)


def expert_partials(hidden, down, named, n_seq, tokens):
    exp_dev, rows, ff_units = hidden.shape
    width = down.shape[2]
    pad = rows // n_seq
    tile = min(width, 512)
    return pl.pallas_call(
        functools.partial(expert_kernel, exp_dev, n_seq, pad),
        grid=(width // tile,),
        out_shape=jax.ShapeDtypeStruct((n_seq, tokens, width), BF16),
        in_specs=[
            pl.BlockSpec((exp_dev, rows, ff_units), lambda n: (0, 0, 0)),
            pl.BlockSpec((exp_dev, ff_units, tile), lambda n: (0, 0, n)),
            pl.BlockSpec(named.shape, lambda n: (0, 0, 0)),
        ],
        out_specs=pl.BlockSpec((n_seq, tokens, tile), lambda n: (0, 0, n)),
        scratch_shapes=[
            pltpu.VMEM((n_seq, tokens, exp_dev * pad), BF16),
            pltpu.VMEM((n_seq, exp_dev * pad, tile), BF16),
        ],
        compiler_params=pltpu.CompilerParams(vmem_limit_bytes=VMEM_BYTES),
        cost_estimate=pl.CostEstimate(
            flops=2 * exp_dev * rows * width * (ff_units + tokens),
            bytes_accessed=2 * (hidden.size + down.size + n_seq * tokens * width),
            transcendentals=0,
        ),
        name="experts",
    )(hidden, down, named)


def sum_decays(decay_ref, decay_t_ref, sum_ref, sum_t_ref):
    tokens = decay_ref.shape[0]
    row, col = iotas(tokens, tokens)
    exact = functools.partial(
        jnp.dot, precision=lax.Precision.HIGHEST, preferred_element_type=F32
    )
    sum_ref[...] = exact((row >= col).astype(F32), decay_ref[...])
    sum_t_ref[...] = exact(decay_t_ref[...], (row <= col).astype(F32))


def unit(x):
    x = x.astype(F32)
    return x * lax.rsqrt(jnp.sum(x * x, axis=-1, keepdims=True) + 1e-06)


def key_head_maps(kh, q, k, rate_ref, rate_t_ref, sum_ref, sum_t_ref):
    tokens = q.shape[0]
    row, col = iotas(tokens, tokens)
    inclusive, strict = row >= col, row > col
    kn = unit(k)
    qn = unit(q) * DK ** (-0.5)
    kn_t = kn.T
    pairs = dot3(jnp.concatenate([kn, qn], axis=0), kn_t)
    kk, qk = pairs[:tokens], pairs[tokens:]
    per = HV // HK
    sums, rates = sum_ref[...], rate_ref[...]
    lane = lax.broadcasted_iota(jnp.int32, sums.shape, 1)
    levels = []
    size = 1
    while size < tokens:
        levels.append(size)
        size *= 2
    state = []
    for u in range(per):
        h = kh * per + u
        s_col = jnp.sum(jnp.where(lane == h, sums, 0.0), axis=1, keepdims=True)
        b_col = jnp.sum(jnp.where(lane == h, rates, 0.0), axis=1, keepdims=True)
        s_row, b_row = sum_t_ref[pl.ds(h, 1), :], rate_t_ref[pl.ds(h, 1), :]
        ratio = jnp.where(inclusive, jnp.exp(jnp.where(inclusive, s_col - s_row, 0.0)), 0.0)
        lower = jnp.where(strict, b_col * ratio * kk, 0.0)
        state.append([s_col, s_row, b_row, ratio, lower, (row == col).astype(F32)])
    for size in levels:
        joins = (row // (2 * size) == col // (2 * size)) & (row // size != col // size)
        for st in state:
            link = jnp.where(joins, st[4], 0.0)
            if size == 1:
                st[5] = st[5] - link
            else:
                st[5] = st[5] - dot3(st[5], dot3(link, st[5]))
    outs = []
    for u, (s_col, s_row, b_row, ratio, lower, inverse) in enumerate(state):
        last = s_row[:, tokens - 1 :]
        growth = jnp.exp(s_col)
        both = jnp.concatenate([qk * ratio, kn_t * jnp.exp(last - s_row)], axis=0)
        mn = dot3(both, inverse) * b_row
        base = jnp.concatenate(
            [growth * qn, jnp.where(row == col, jnp.exp(last), 0.0)], axis=0
        )
        ga = base - dot3(mn, growth * kn)
        outs.append((mn.astype(BF16), ga.astype(BF16)))
    return outs


def maps_kernel(q_ref, k_ref, decay_ref, decay_t_ref, rate_ref, rate_t_ref, mn_ref, ga_ref, sum_ref, sum_t_ref):
    kh = pl.program_id(0)

    @pl.when(kh == 0)
    def _():
        sum_decays(decay_ref, decay_t_ref, sum_ref, sum_t_ref)

    outs = key_head_maps(kh, q_ref[...], k_ref[...], rate_ref, rate_t_ref, sum_ref, sum_t_ref)
    for u, (mn, ga) in enumerate(outs):
        mn_ref[u] = mn
        ga_ref[u] = ga


def head_maps(queries, keys, decay, rate):
    tokens = queries.shape[0]
    per = HV // HK
    whole = lambda shape: pl.BlockSpec(shape, lambda h: (0, 0))
    out = jax.ShapeDtypeStruct((HV, tokens + DK, DK), BF16)
    return pl.pallas_call(
        maps_kernel,
        grid=(HK,),
        out_shape=(out, out),
        in_specs=[
            pl.BlockSpec((tokens, DK), lambda h: (0, h)),
            pl.BlockSpec((tokens, DK), lambda h: (0, h)),
            whole((tokens, HV)),
            whole((HV, tokens)),
            whole((tokens, HV)),
            whole((HV, tokens)),
        ],
        out_specs=[pl.BlockSpec((per, tokens + DK, DK), lambda h: (h, 0, 0))] * 2,
        scratch_shapes=[pltpu.VMEM((tokens, HV), F32), pltpu.VMEM((HV, tokens), F32)],
        compiler_params=pltpu.CompilerParams(vmem_limit_bytes=VMEM_BYTES),
        cost_estimate=pl.CostEstimate(
            flops=HV * 64 * 2 * tokens * tokens * DK,
            bytes_accessed=6 * tokens * HV * DK * 2,
            transcendentals=HV * tokens * tokens,
        ),
        name="maps",
    )(queries, keys, decay, decay.T, rate, rate.T)


def value_kernel(res_ref, moe_ref, gain_ref, weight_ref, mn_ref, out_ref, state_ref, normed_ref):
    tokens = res_ref.shape[0]

    @pl.when(pl.program_id(0) == 0)
    def _():
        stream = (res_ref[...].astype(F32) + moe_ref[...].astype(F32)).astype(BF16).astype(F32)
        scale = lax.rsqrt(jnp.mean(stream * stream, axis=-1, keepdims=True) + 1e-06)
        normed_ref[...] = (stream * scale * gain_ref[...].astype(F32)).astype(BF16)

    values = jnp.dot(normed_ref[...], weight_ref[...], preferred_element_type=F32).astype(BF16)
    for u in range(mn_ref.shape[0]):
        both = jnp.dot(
            mn_ref[u], values[:, u * DV : (u + 1) * DV], preferred_element_type=F32
        )
        out_ref[:, u * DV : (u + 1) * DV] = both[:tokens]
        state_ref[u] = both[tokens:].astype(BF16)


def value_heads(residual, moe, gain, weight, mn):
    tokens, width = residual.shape
    per = 4
    tile = per * DV
    whole = lambda shape: pl.BlockSpec(shape, lambda n: (0, 0))
    return pl.pallas_call(
        value_kernel,
        grid=(HV // per,),
        out_shape=(
            jax.ShapeDtypeStruct((tokens, HV * DV), F32),
            jax.ShapeDtypeStruct((HV, DK, DV), BF16),
        ),
        in_specs=[
            whole((tokens, width)),
            whole((tokens, width)),
            whole((1, width)),
            pl.BlockSpec((width, tile), lambda n: (0, n)),
            pl.BlockSpec((per, tokens + DK, DK), lambda n: (n, 0, 0)),
        ],
        out_specs=[
            pl.BlockSpec((tokens, tile), lambda n: (0, n)),
            pl.BlockSpec((per, DK, DV), lambda n: (n, 0, 0)),
        ],
        scratch_shapes=[pltpu.VMEM((tokens, width), BF16)],
        compiler_params=pltpu.CompilerParams(vmem_limit_bytes=VMEM_BYTES),
        cost_estimate=pl.CostEstimate(
            flops=2 * tokens * width * HV * DV,
            bytes_accessed=2 * (weight.size + 6 * tokens * width),
            transcendentals=0,
        ),
        name="values",
    )(residual, moe, gain.reshape(1, width), weight, mn)


def close_kernel(maps_ref, states_ref, ga_ref, zero_ref, out_ref):
    n_sa, per = maps_ref.shape[:2]
    tokens = zero_ref.shape[0]
    here = lax.axis_index("sa")
    for u in range(per):
        state = jnp.zeros((DK, DV), F32)
        for i in range(n_sa - 1):
            new = states_ref[i, u].astype(F32)
            if i > 0:
                new = new + dot1(maps_ref[i, u], state)
            state = jnp.where(i < here, new, state)
        cols = slice(u * DV, (u + 1) * DV)
        out_ref[:, cols] = (zero_ref[:, cols] + dot1(ga_ref[u, :tokens], state)).astype(BF16)


def close_heads(maps, states, ga, zero):
    n_sa = maps.shape[0]
    tokens = zero.shape[0]
    per = 4
    gathered = pl.BlockSpec((n_sa, per, DK, DK), lambda n: (0, n, 0, 0))
    return pl.pallas_call(
        close_kernel,
        grid=(HV // per,),
        out_shape=jax.ShapeDtypeStruct((tokens, HV * DV), BF16),
        in_specs=[
            gathered,
            gathered,
            pl.BlockSpec((per, tokens + DK, DK), lambda n: (n, 0, 0)),
            pl.BlockSpec((tokens, per * DV), lambda n: (0, n)),
        ],
        out_specs=pl.BlockSpec((tokens, per * DV), lambda n: (0, n)),
        compiler_params=pltpu.CompilerParams(vmem_limit_bytes=VMEM_BYTES),
        cost_estimate=pl.CostEstimate(
            flops=HV * n_sa * 2 * DK * DK * DV,
            bytes_accessed=2 * (2 * maps.size + ga.size + 3 * zero.size),
            transcendentals=0,
        ),
        name="close",
    )(maps, states, ga, zero)


def gather_kernel(
    cap, pad,
    named_ref, hidden_hbm, down_hbm, res_ref, gain_ref, weight_ref, q_ref, k_ref,
    decay_ref, decay_t_ref, rate_ref, rate_t_ref,
    normed_ref, full_ref, mn_ref, ga_ref,
    table_ref, hidden_ref, down_ref, made_ref, mix_ref, send_ref, got_ref, mate_ref, sum_ref, sum_t_ref,
    load_sem, own_sem, sem_t, sem_w, sem_f, sem_y, sem_g, sem_m, sem_p,
):
    n = lax.axis_size("ea")
    me, here = lax.axis_index("ea"), lax.axis_index("sa")
    partner = here + 1 - 2 * lax.rem(here, 2)
    across = lax.rem(here + 2, 4)
    part = weight_ref.shape[0] // 4
    mine = pl.ds(pl.multiple_of(here * part, part), part)
    others = pl.ds(pl.multiple_of(across * part, part), part)
    lines, line, side = n // 2, me // 2, lax.rem(me, 2)
    mate = line * 2 + 1 - side
    exp_dev, tokens, width = down_hbm.shape[0], res_ref.shape[0], res_ref.shape[1]
    top = named_ref.shape[0] // 2
    tile = 512
    tiles = width // tile

    def peer(d):
        return lax.rem(me + d, n)

    def origin(d):
        return lax.rem(me + n - d, n)

    def remote(src, dst, sems, d, where):
        return pltpu.make_async_remote_copy(
            src_ref=src, dst_ref=dst, send_sem=sems.at[0, d], recv_sem=sems.at[1, d],
            device_id=where, device_id_type=MESH,
        )

    def table_copy(d):
        return remote(named_ref, table_ref.at[me], sem_t, d, {"ea": peer(d)})

    def weight_copy(d):
        return remote(weight_ref.at[mine], full_ref.at[me, mine], sem_w, d, {"ea": peer(d)})

    def forward_copy(d):
        block = full_ref.at[origin(d), mine]
        return remote(block, block, sem_f, d, {"sa": partner})

    def across_copy(d):
        block = full_ref.at[origin(d), mine]
        return remote(block, block, sem_y, d, {"sa": across})

    def second_copy(d):
        block = full_ref.at[origin(d), others]
        return remote(block, block, sem_g, d, {"sa": partner})

    def beyond(i):
        return lax.rem(line + 1 + i, lines) * 2

    def mate_copy(i):
        return remote(send_ref.at[beyond(i) + 1 - side], mate_ref.at[i], sem_m, i, {"ea": mate})

    def partial_copy(i):
        there = beyond(i) + side
        return remote(send_ref.at[there], got_ref.at[i], sem_p, i, {"ea": there})

    def each(action):
        def turn(d, carry):
            action(d)
            return carry

        lax.fori_loop(1, n, turn, 0)

    loads = []
    for e in range(exp_dev):
        loads.append((
            pltpu.make_async_copy(hidden_hbm.at[e], hidden_ref.at[e], load_sem.at[0, e]),
            pltpu.make_async_copy(down_hbm.at[e], down_ref.at[e], load_sem.at[1, e]),
        ))
        for copy in loads[-1]:
            copy.start()
    own = pltpu.make_async_copy(weight_ref, full_ref.at[me], own_sem)
    own.start()

    barrier = pltpu.get_barrier_semaphore()
    each(lambda d: pl.semaphore_signal(barrier, inc=1, device_id={"ea": peer(d)}, device_id_type=MESH))
    pl.semaphore_signal(barrier, inc=1, device_id={"sa": partner}, device_id_type=MESH)
    pl.semaphore_signal(barrier, inc=1, device_id={"sa": across}, device_id_type=MESH)
    pl.semaphore_wait(barrier, n + 1)

    each(lambda d: table_copy(d).start())
    each(lambda d: weight_copy(d).start())

    for e in range(exp_dev):
        for copy in loads[e]:
            copy.wait()
        if pad > cap:
            made_ref[:, e * pad + cap : (e + 1) * pad, :] = jnp.zeros((n, pad - cap, width), BF16)

        def project(t, carry):
            cols = pl.ds(pl.multiple_of(t * tile, tile), tile)
            made = jnp.dot(hidden_ref[e], down_ref[e, :, cols], preferred_element_type=F32)
            for s in range(n):
                made_ref[s, e * pad : e * pad + cap, cols] = made[s * cap : (s + 1) * cap].astype(BF16)
            return carry

        lax.fori_loop(0, tiles, project, 0)

    table_ref[me] = named_ref[...]
    row, col = iotas(tokens, tokens)
    after = (row < col).astype(BF16)
    place = lax.broadcasted_iota(jnp.int32, (pad, tokens), 0).astype(F32)

    each(lambda d: table_copy(d).wait_recv())

    def mixing(s):
        named = table_ref[s]
        ids, weights = named[:top], named[top:]
        parts = []
        for e in range(exp_dev):
            hit = ids == (me * exp_dev + e).astype(F32)
            count = jnp.sum(hit.astype(F32), axis=0, keepdims=True)
            weight = jnp.sum(jnp.where(hit, weights, 0.0), axis=0, keepdims=True)
            slot = jnp.dot(
                jnp.broadcast_to(count, (pad, tokens)).astype(BF16), after, preferred_element_type=F32
            )
            parts.append(jnp.where((slot == place) & (count > 0.0), weight, 0.0))
        mix_ref[...] = jnp.concatenate(parts, axis=0).T.astype(BF16)

    def combine(s, extra):
        mixing(s)

        def block(t, inner):
            cols = pl.ds(pl.multiple_of(t * tile, tile), tile)
            total = jnp.dot(mix_ref[...], made_ref[s, :, cols], preferred_element_type=F32)
            if extra is not None:
                total = total + mate_ref[extra, :, cols].astype(F32)
            send_ref[s, :, cols] = total.astype(BF16)
            return inner

        lax.fori_loop(0, tiles, block, 0)

    def to_mate(i, carry):
        combine(beyond(i) + 1 - side, None)
        mate_copy(i).start()
        return carry

    lax.fori_loop(0, lines, to_mate, 0)

    def pass_on(d):
        weight_copy(d).wait_recv()
        across_copy(d).start()
        forward_copy(d).start()

    sum_decays(decay_ref, decay_t_ref, sum_ref, sum_t_ref)

    def maps(kh, carry):
        cols = pl.ds(pl.multiple_of(kh * DK, DK), DK)
        outs = key_head_maps(kh, q_ref[:, cols], k_ref[:, cols], rate_ref, rate_t_ref, sum_ref, sum_t_ref)
        for u, (mn, ga) in enumerate(outs):
            mn_ref[kh * (HV // HK) + u] = mn
            ga_ref[kh * (HV // HK) + u] = ga

        @pl.when(kh + 1 < n)
        def _():
            pass_on(kh + 1)

        return carry

    lax.fori_loop(0, HK, maps, 0)
    for d in range(HK + 1, n):
        pass_on(d)

    def along(i, carry):
        mate_copy(i).wait_recv()
        combine(beyond(i) + side, i)

        @pl.when(i < lines - 1)
        def _():
            partial_copy(i).start()

        return carry

    lax.fori_loop(0, lines, along, 0)

    def pass_second(d):
        across_copy(d).wait_recv()
        second_copy(d).start()

    each(pass_second)
    for i in range(lines - 1):
        partial_copy(i).wait_recv()

    def close(r, carry):
        rows = pl.ds(pl.multiple_of(r * 16, 16), 16)
        moe = send_ref[me, rows, :].astype(F32)
        for d in range(lines - 1):
            moe = moe + got_ref[d, rows, :].astype(F32)
        stream = (res_ref[rows, :].astype(F32) + moe).astype(BF16).astype(F32)
        scale = lax.rsqrt(jnp.mean(stream * stream, axis=-1, keepdims=True) + 1e-06)
        normed_ref[rows, :] = (stream * scale * gain_ref[...].astype(F32)).astype(BF16)
        return carry

    lax.fori_loop(0, tokens // 16, close, 0)
    own.wait()

    def finish(d):
        forward_copy(d).wait()
        table_copy(d).wait_send()
        weight_copy(d).wait_send()
        across_copy(d).wait_send()
        second_copy(d).wait()

    each(finish)
    for i in range(lines):
        mate_copy(i).wait_send()
        if i < lines - 1:
            partial_copy(i).wait_send()


def gather_stage(n, named, hidden, down, residual, gain, weight, queries, keys, decay, rate):
    exp_dev, rows, ff_units = hidden.shape
    tokens, width = residual.shape
    cap = rows // n
    pad = -(-cap // 16) * 16
    vmem = pl.BlockSpec(memory_space=pltpu.VMEM)
    hbm = pl.BlockSpec(memory_space=pl.ANY)
    maps = jax.ShapeDtypeStruct((HV, tokens + DK, DK), BF16)
    dma = pltpu.SemaphoreType.DMA
    return pl.pallas_call(
        functools.partial(gather_kernel, cap, pad),
        out_shape=(
            jax.ShapeDtypeStruct((tokens, width), BF16),
            jax.ShapeDtypeStruct((n,) + weight.shape, BF16),
            maps,
            maps,
        ),
        in_specs=[vmem, hbm, hbm] + [vmem] * 9,
        out_specs=[vmem, hbm, vmem, vmem],
        scratch_shapes=[
            pltpu.VMEM((n,) + named.shape, F32),
            pltpu.VMEM(hidden.shape, BF16),
            pltpu.VMEM(down.shape, BF16),
            pltpu.VMEM((n, exp_dev * pad, width), BF16),
            pltpu.VMEM((tokens, exp_dev * pad), BF16),
            pltpu.VMEM((n, tokens, width), BF16),
            pltpu.VMEM((max(n // 2 - 1, 1), tokens, width), BF16),
            pltpu.VMEM((n // 2, tokens, width), BF16),
            pltpu.VMEM((tokens, HV), F32),
            pltpu.VMEM((HV, tokens), F32),
            dma((2, exp_dev)),
            dma,
            dma((2, n)),
            dma((2, n)),
            dma((2, n)),
            dma((2, n)),
            dma((2, n)),
            dma((2, n // 2)),
            dma((2, n // 2)),
        ],
        compiler_params=pltpu.CompilerParams(
            vmem_limit_bytes=VMEM_BYTES, collective_id=0, has_side_effects=True
        ),
        name="gather",
    )(named, hidden, down, residual, gain.reshape(1, width), weight, queries, keys, decay, decay.T, rate, rate.T)


def chain_kernel(normed_ref, weight_ref, mn_ref, ga_ref, out_ref, send_ref, got_ref, sem):
    g, groups = pl.program_id(0), pl.num_programs(0)
    n, here = lax.axis_size("sa"), lax.axis_index("sa")
    tokens = normed_ref.shape[0]
    per = mn_ref.shape[0]
    following, previous = lax.rem(here + 1, n), lax.rem(here + n - 1, n)

    @pl.when(g == 0)
    def _():
        barrier = pltpu.get_barrier_semaphore()
        for where in (following, previous):
            pl.semaphore_signal(barrier, inc=1, device_id={"sa": where}, device_id_type=MESH)
        pl.semaphore_wait(barrier, 2)
        got_ref_first = jnp.zeros(got_ref.shape[1:], BF16)

        @pl.when(here == 0)
        def _():
            for i in range(got_ref.shape[0]):
                got_ref[i] = got_ref_first

    def copy(i):
        return pltpu.make_async_remote_copy(
            src_ref=send_ref.at[i], dst_ref=got_ref.at[i], send_sem=sem.at[0, i],
            recv_sem=sem.at[1, i], device_id={"sa": following}, device_id_type=MESH,
        )

    values = jnp.dot(normed_ref[...], weight_ref[...], preferred_element_type=F32).astype(BF16)
    both = [
        jnp.dot(mn_ref[u], values[:, u * DV : (u + 1) * DV], preferred_element_type=F32)
        for u in range(per)
    ]

    @pl.when(here > 0)
    def _():
        copy(g).wait_recv()

    after = [
        both[u] + jnp.dot(ga_ref[u], got_ref[g, u], preferred_element_type=F32) for u in range(per)
    ]
    for u in range(per):
        send_ref[g, u] = after[u][tokens:].astype(BF16)

    @pl.when(here < n - 1)
    def _():
        copy(g).start()

    for u in range(per):
        out_ref[:, u * DV : (u + 1) * DV] = after[u][:tokens].astype(BF16)

    @pl.when((g == groups - 1) & (here < n - 1))
    def _():
        for i in range(send_ref.shape[0]):
            copy(i).wait_send()


def chain_stage(normed, weight, mn, ga):
    tokens, width = normed.shape
    per = 4
    groups = HV // per
    tile = per * DV
    states = pltpu.VMEM((groups, per, DK, DV), BF16)
    maps = pl.BlockSpec((per, tokens + DK, DK), lambda g: (g, 0, 0))
    return pl.pallas_call(
        chain_kernel,
        grid=(groups,),
        out_shape=jax.ShapeDtypeStruct((tokens, HV * DV), BF16),
        in_specs=[
            pl.BlockSpec((tokens, width), lambda g: (0, 0)),
            pl.BlockSpec((width, tile), lambda g: (0, g)),
            maps,
            maps,
        ],
        out_specs=pl.BlockSpec((tokens, tile), lambda g: (0, g)),
        scratch_shapes=[states, states, pltpu.SemaphoreType.DMA((2, groups))],
        compiler_params=pltpu.CompilerParams(
            vmem_limit_bytes=VMEM_BYTES, collective_id=1, has_side_effects=True
        ),
        name="chain",
    )(normed, weight, mn, ga)


def on_device(
    expert_hidden,
    down_weight,
    residual,
    expert_ids,
    combine_weight,
    norm_gain,
    value_weight,
    queries,
    keys,
    log_decay,
    write_rate,
):
    n_ea = lax.axis_size("ea")
    exp_dev, rows, ff_units = expert_hidden.shape
    cap = rows // n_ea
    tokens = residual.shape[1]
    named = jnp.concatenate([expert_ids[0].astype(F32), combine_weight[0]], axis=-1)
    fits = n_ea * tokens * residual.shape[2] <= 4 * 1024 * 1024 and cap % 8 == 0
    if fits and n_ea % 2 == 0 and lax.axis_size("sa") == 4:
        normed, weight, mn, ga = gather_stage(
            n_ea, named.T, expert_hidden, down_weight, residual[0], norm_gain, value_weight,
            queries[0], keys[0], log_decay[0], write_rate[0],
        )
        return chain_stage(normed, weight.reshape(-1, weight.shape[2]), mn, ga)[None]
    pad = -(-cap // 16) * 16
    hidden = jnp.pad(
        expert_hidden.reshape(exp_dev, n_ea, cap, ff_units), ((0, 0), (0, 0), (0, pad - cap), (0, 0))
    ).reshape(exp_dev, n_ea * pad, ff_units)
    named = lax.all_gather(named, "ea")
    weight = lax.all_gather(value_weight, "ea", axis=0, tiled=True)
    partial = expert_partials(hidden, down_weight, named, n_ea, tokens)
    moe = lax.psum_scatter(partial, "ea", scatter_dimension=0, tiled=True)[0]
    mn, ga = head_maps(queries[0], keys[0], log_decay[0], write_rate[0])
    maps = lax.all_gather(ga[:, tokens:], "sa")
    zero, state = value_heads(residual[0], moe, norm_gain, weight, mn)
    states = lax.all_gather(state, "sa")
    return close_heads(maps, states, ga, zero)[None]


def solution(mesh):
    return jax.shard_map(
        on_device,
        mesh=mesh,
        in_specs=(
            P("ea", "sa", None),
            P("ea", None, None),
            P("ea", "sa", None),
            P("ea", "sa", None),
            P("ea", "sa", None),
            P(),
            P("ea", None),
            P("ea", "sa", None),
            P("ea", "sa", None),
            P("ea", "sa", None),
            P("ea", "sa", None),
        ),
        out_specs=P("ea", "sa", None),
        check_vma=False,
    )
```
